32 devices in a mesh: tm: 4 (over x, core), batch: 8 (over z, y).
Axes of the slice: x: 2, y: 2, z: 4, core: 2. Of those that a mesh axis runs over, the one named last changes fastest.
Arguments:
- latents: float32 [8, 16, 4096], P('tm', None, 'batch'), may hold values from -6 to 6
- shifts: int32 [16], replicated, may hold values from 0 to 7
- starts: int32 [16], replicated, may hold values from 0 to 2
- labels: int32 [16], replicated, may hold values from 0 to 1000
- class_table: bfloat16 [1001, 1152], replicated, may hold values from -6 to 6
- w_freq: bfloat16 [256, 1152], replicated, may hold values from -0.375 to 0.375
- w_time: bfloat16 [1152, 1152], replicated, may hold values from -0.1875 to 0.1875
- w_ada: bfloat16 [1152, 9216], P(None, 'tm'), may hold values from -0.1875 to 0.1875
- w_patch: bfloat16 [16, 1152], replicated, may hold values from -1.5 to 1.5
- w_qkv: bfloat16 [1152, 3456], P('batch', 'tm'), may hold values from -1 to 1
- w_proj: bfloat16 [1152, 1152], P('tm', 'batch'), may hold values from -0.1875 to 0.1875
- w_fc1: bfloat16 [1152, 4608], P('batch', 'tm'), may hold values from -0.1875 to 0.1875
- w_fc2: bfloat16 [4608, 1152], P('tm', 'batch'), may hold values from -0.09375 to 0.09375
- w_final: bfloat16 [1152, 16], replicated, may hold values from -0.1875 to 0.1875
Outputs:
- new_latents: float32 [8, 16, 4096], P('tm', None, 'batch')
- velocity: bfloat16 [8, 16, 4096], P('tm', None, 'batch')
The draws below stay inside these ranges and needn't reach their ends.
All inputs are finite; a program needn't handle non-finite values.
Results may differ from the reference program's by a relative error of at most 0.0091.
Values may be sent and summed in bfloat16 or wider, within the bound.
A program may use at most 128 MiB of HBM per device.

```python
import math
import jax
import jax.numpy as jnp
from jax import lax

D = 1152
HEADS = 16
FF = 4608
FREQ = 256
NCLASS = 1001
GRID = 16
WIN = 8
STEPS = 18
BATCH = 16
LAT = 4096


def draw_w_qkv(key, part):
    base_key = jax.random.fold_in(key, 0)
    head_size = D // HEADS
    base = jax.random.truncated_normal(base_key, -6.0, 6.0, (D, HEADS, 3, head_size), jnp.float32) / math.sqrt(D)
    return jnp.clip(base, -1.0, 1.0).reshape(D, 3 * D).astype(jnp.bfloat16)


def set_ends(entries, own_key, smallest, high):
    longest = entries.shape.index(max(entries.shape))
    spots = []
    for shift in (0, 1):
        where = [jax.random.randint(jax.random.fold_in(own_key, axis), (), 0, length) for axis, length in enumerate(entries.shape)]
        where[longest] = (where[longest] + shift) % entries.shape[longest]
        spots.append(tuple(where))
    return entries.at[spots[0]].set(smallest).at[spots[1]].set(high)


def block_levels(key, shape, shards, low, top_value):
    factor_of = 1.0
    for dim, blocks in shards:
        steps = jax.random.uniform(jax.random.fold_in(jax.random.fold_in(key, 6), dim), (blocks,), jnp.float32, low / len(shards), top_value / len(shards))
        factor_of = factor_of * jnp.repeat(jnp.exp(steps), shape[dim] // blocks).reshape((-1,) + (1,) * (len(shape) - 1 - dim))
    return factor_of


def gaussian(key, shape, deviation, bound, shards=(), held_as=jnp.bfloat16):
    loudness = block_levels(key, shape, shards, -0.22, 0.18) if shards else 1.0
    entries = jax.random.normal(key, shape, jnp.float32) * deviation * loudness
    return jnp.minimum(jnp.maximum(entries, -bound), bound).astype(held_as)


def setup_inputs(seed: int = 0) -> dict:
    arg_keys = jax.random.split(jax.random.key(seed), 15)
    latents = gaussian(arg_keys[0], (WIN, BATCH, LAT), 1.0, 6.0, ((0, 4), (2, 8)), jnp.float32)
    shifts = set_ends(jax.random.randint(arg_keys[1], (BATCH,), 0, WIN), jax.random.fold_in(arg_keys[1], 1), 0, WIN - 1).astype(jnp.int32)
    starts = set_ends(jax.random.randint(arg_keys[2], (BATCH,), 0, STEPS - 2 * WIN + 1), jax.random.fold_in(arg_keys[2], 1), 0, STEPS - 2 * WIN).astype(jnp.int32)
    labels = set_ends(jax.random.randint(arg_keys[3], (BATCH,), 0, NCLASS), jax.random.fold_in(arg_keys[3], 1), 0, NCLASS - 1).astype(jnp.int32)
    class_table = gaussian(arg_keys[4], (NCLASS, D), 1.0, 6.0)
    w_freq = gaussian(arg_keys[5], (FREQ, D), FREQ ** -0.5, 0.375)
    w_time = gaussian(arg_keys[6], (D, D), D ** -0.5, 0.1875)
    w_ada = gaussian(arg_keys[7], (D, 8 * D), D ** -0.5, 0.1875, ((1, 4),))
    w_patch = gaussian(arg_keys[8], (16, D), 16 ** -0.5, 1.5)
    w_qkv = draw_w_qkv(jax.random.fold_in(arg_keys[14], 71), 0)
    w_proj = gaussian(arg_keys[10], (D, D), D ** -0.5, 0.1875, ((0, 4), (1, 8)))
    w_fc1 = gaussian(arg_keys[11], (D, FF), D ** -0.5, 0.1875, ((0, 8), (1, 4)))
    w_fc2 = gaussian(arg_keys[12], (FF, D), FF ** -0.5, 0.09375, ((0, 4), (1, 8)))
    w_final = gaussian(arg_keys[13], (D, 16), D ** -0.5, 0.1875)
    return dict(latents=latents, shifts=shifts, starts=starts, labels=labels, class_table=class_table, w_freq=w_freq, w_time=w_time, w_ada=w_ada, w_patch=w_patch, w_qkv=w_qkv, w_proj=w_proj, w_fc1=w_fc1, w_fc2=w_fc2, w_final=w_final)


def layer_norm(values):
    average = lax.optimization_barrier(jnp.mean(values, axis=-1, keepdims=True))
    centred = values - average
    variance = lax.optimization_barrier(jnp.mean(centred * centred, axis=-1, keepdims=True))
    return centred * lax.rsqrt(variance + 1e-06)

def position_table(token_count):
    token_ids = jnp.arange(token_count, dtype=jnp.int32)
    row_ids = (token_ids // GRID).astype(jnp.float32)
    col_ids = (token_ids % GRID).astype(jnp.float32)
    quarter = D // 4
    omegas = jnp.exp(-math.log(10000.0) * jnp.arange(quarter, dtype=jnp.float32) / quarter)
    col_angle = col_ids[:, None] * omegas[None, :]
    row_angle = row_ids[:, None] * omegas[None, :]
    return jnp.concatenate([jnp.sin(col_angle), jnp.cos(col_angle), jnp.sin(row_angle), jnp.cos(row_angle)], axis=1)

def cond_activation(step_ids, class_ids, class_table, w_freq, w_time):
    half_freq = FREQ // 2
    freqs = jnp.exp(-math.log(10000.0) * jnp.arange(half_freq, dtype=jnp.float32) / half_freq)
    tvalue = 1000.0 * (1.0 - step_ids.astype(jnp.float32) / STEPS)
    angles = tvalue[:, None] * freqs[None, :]
    embedded = jnp.concatenate([jnp.cos(angles), jnp.sin(angles)], axis=1).astype(jnp.bfloat16)
    hidden_time = jax.nn.silu(jnp.dot(embedded, w_freq, preferred_element_type=jnp.float32)).astype(jnp.bfloat16)
    condition = jnp.dot(hidden_time, w_time, preferred_element_type=jnp.float32) + jnp.take(class_table, class_ids, axis=0).astype(jnp.float32)
    return jax.nn.silu(condition).astype(jnp.bfloat16)

def attend(qkv_rows):
    token_count = qkv_rows.shape[0]
    head_size = D // HEADS
    grouped = qkv_rows.reshape(token_count, HEADS, 3, head_size)
    query = grouped[:, :, 0, :].astype(jnp.float32)
    keys = grouped[:, :, 1, :].astype(jnp.float32)
    values = grouped[:, :, 2, :].astype(jnp.float32)
    scores = jnp.einsum('qhd,khd->hqk', query, keys) * (1.0 / math.sqrt(head_size))
    peak = lax.optimization_barrier(jnp.max(scores, axis=-1, keepdims=True))
    weights = jnp.exp(scores - peak)
    weights = weights / lax.optimization_barrier(jnp.sum(weights, axis=-1, keepdims=True))
    rounded = lax.optimization_barrier(weights.astype(jnp.bfloat16))
    attended = jnp.einsum('hqk,khd->qhd', rounded.astype(jnp.float32), values)
    return attended.astype(jnp.bfloat16).reshape(token_count, HEADS * head_size)

def denoise(point_row, modulation, w_patch, w_qkv, w_proj, w_fc1, w_fc2, w_final):
    patch_size = w_patch.shape[0]
    token_count = point_row.shape[0] // patch_size
    patch_in = point_row.reshape(token_count, patch_size).astype(jnp.bfloat16)
    tokens = jnp.dot(patch_in, w_patch, preferred_element_type=jnp.float32) + position_table(token_count)
    mod_float = modulation.astype(jnp.float32)
    mod_parts = [mod_float[block_index * D:(block_index + 1) * D][None, :] for block_index in range(8)]
    normed = (layer_norm(tokens) * (1.0 + mod_parts[1]) + mod_parts[0]).astype(jnp.bfloat16)
    qkv_rows = jnp.dot(normed, w_qkv, preferred_element_type=jnp.float32).astype(jnp.bfloat16)
    attended = attend(qkv_rows)
    mixed = tokens + mod_parts[2] * jnp.dot(attended, w_proj, preferred_element_type=jnp.float32)
    normed_two = (layer_norm(mixed) * (1.0 + mod_parts[4]) + mod_parts[3]).astype(jnp.bfloat16)
    hidden_units = jax.nn.gelu(jnp.dot(normed_two, w_fc1, preferred_element_type=jnp.float32), approximate=True).astype(jnp.bfloat16)
    residual = mixed + mod_parts[5] * jnp.dot(hidden_units, w_fc2, preferred_element_type=jnp.float32)
    final_in = (layer_norm(residual) * (1.0 + mod_parts[7]) + mod_parts[6]).astype(jnp.bfloat16)
    return jnp.dot(final_in, w_final, preferred_element_type=jnp.float32).astype(jnp.bfloat16).reshape(-1)

def reference(latents, shifts, starts, labels, class_table, w_freq, w_time, w_ada, w_patch, w_qkv, w_proj, w_fc1, w_fc2, w_final):
    positions = jnp.arange(WIN, dtype=jnp.int32)[:, None]
    source_rows = jnp.minimum(positions + shifts[None, :], WIN - 1).astype(jnp.int32)
    points = jnp.take_along_axis(latents, source_rows[:, :, None], axis=0)
    step_ids = (starts + shifts)[None, :] + positions
    class_ids = jnp.broadcast_to(labels[None, :], (WIN, BATCH))
    activation = cond_activation(step_ids.reshape(-1), class_ids.reshape(-1), class_table, w_freq, w_time)
    modulation = jnp.dot(activation, w_ada, preferred_element_type=jnp.float32).astype(jnp.bfloat16)

    def one_point(paired):
        return denoise(paired[0], paired[1], w_patch, w_qkv, w_proj, w_fc1, w_fc2, w_final)
    velocity = lax.map(one_point, (points.reshape(WIN * BATCH, LAT), modulation)).reshape(WIN, BATCH, LAT)
    velocity_float = velocity.astype(jnp.float32)
    summed = jnp.cumsum(velocity_float, axis=0)
    running = jnp.concatenate([jnp.zeros_like(summed[:1]), summed[:-1]], axis=0)
    new_latents = points[0][None] + running * (1.0 / STEPS)
    return (new_latents, velocity)
```

```python
import functools
import math

import jax
import jax.numpy as jnp
from jax import lax
from jax.experimental import pallas as pl
from jax.sharding import PartitionSpec as P

D = 1152
HEADS = 16
FREQ = 256
GRID = 16
STEPS = 18


def entering(part, axis, combine, identity):
    place = lax.axis_index(axis)
    gathered = lax.all_gather(part, axis)
    state = jnp.zeros_like(part) + jnp.asarray(identity, part.dtype)

    def one(lap, state):
        return combine(state, lax.dynamic_index_in_dim(gathered, lap, 0, False))

    return lax.fori_loop(0, place, one, state)


def layer_norm(values):
    average = jnp.mean(values, axis=-1, keepdims=True)
    centred = values - average
    variance = jnp.mean(centred * centred, axis=-1, keepdims=True)
    return centred * lax.rsqrt(variance + 1e-06)


def position_table(token_count):
    token_ids = jnp.arange(token_count, dtype=jnp.int32)
    row_ids = (token_ids // GRID).astype(jnp.float32)
    col_ids = (token_ids % GRID).astype(jnp.float32)
    quarter = D // 4
    omegas = jnp.exp(-math.log(10000.0) * jnp.arange(quarter, dtype=jnp.float32) / quarter)
    col_angle = col_ids[:, None] * omegas[None, :]
    row_angle = row_ids[:, None] * omegas[None, :]
    return jnp.concatenate(
        [jnp.sin(col_angle), jnp.cos(col_angle), jnp.sin(row_angle), jnp.cos(row_angle)], axis=1
    )


def cond_activation(step_ids, class_ids, class_table, w_freq, w_time):
    half_freq = FREQ // 2
    freqs = jnp.exp(-math.log(10000.0) * jnp.arange(half_freq, dtype=jnp.float32) / half_freq)
    tvalue = 1000.0 * (1.0 - step_ids.astype(jnp.float32) / STEPS)
    angles = tvalue[:, None] * freqs[None, :]
    embedded = jnp.concatenate([jnp.cos(angles), jnp.sin(angles)], axis=1).astype(jnp.bfloat16)
    hidden_time = jax.nn.silu(jnp.dot(embedded, w_freq, preferred_element_type=jnp.float32)).astype(
        jnp.bfloat16
    )
    condition = jnp.dot(hidden_time, w_time, preferred_element_type=jnp.float32) + jnp.take(
        class_table, class_ids, axis=0
    ).astype(jnp.float32)
    return jax.nn.silu(condition).astype(jnp.bfloat16)


def attention_kernel(head_count, first, normed_ref, qkv_ref, proj_ref, *rest):
    acc_ref, out_ref = (None, rest[0]) if first else rest
    head_size = proj_ref.shape[0] // head_count
    rows = jnp.dot(normed_ref[0], qkv_ref[...], preferred_element_type=jnp.float32)
    rows = rows.astype(jnp.bfloat16)
    scale = 1.0 / math.sqrt(head_size)
    pieces = []
    for head in range(head_count):
        start = head * 3 * head_size
        query = rows[:, start : start + head_size]
        keys = rows[:, start + head_size : start + 2 * head_size]
        values = rows[:, start + 2 * head_size : start + 3 * head_size]
        scores = lax.dot_general(
            query, keys, (((1,), (1,)), ((), ())), preferred_element_type=jnp.float32
        )
        peak = jnp.max(scores, axis=-1, keepdims=True)
        weights = jnp.exp((scores - peak) * scale)
        total = jnp.sum(weights, axis=-1, keepdims=True)
        mixed = jnp.dot(
            weights.astype(jnp.bfloat16), values, preferred_element_type=jnp.float32
        )
        pieces.append((mixed / total).astype(jnp.bfloat16))
    attended = jnp.concatenate(pieces, axis=1)
    product = jnp.dot(attended, proj_ref[...], preferred_element_type=jnp.float32)
    out_ref[0] = product if first else acc_ref[0] + product


def mlp_kernel(first, normed_ref, fc1_ref, fc2_ref, *rest):
    acc_ref, out_ref = (None, rest[0]) if first else rest
    hidden = jnp.dot(normed_ref[0], fc1_ref[...], preferred_element_type=jnp.float32)
    hidden = jax.nn.gelu(hidden, approximate=True).astype(jnp.bfloat16)
    product = jnp.dot(hidden, fc2_ref[...], preferred_element_type=jnp.float32)
    out_ref[0] = product if first else acc_ref[0] + product


def shard_call(kernel, normed, first_weight, second_weight, acc, name, flops):
    points, tokens, width = normed.shape
    out_width = second_weight.shape[1]
    by_point = pl.BlockSpec((1, tokens, width), lambda i: (i, 0, 0))
    out_point = pl.BlockSpec((1, tokens, out_width), lambda i: (i, 0, 0))
    operands = [normed, first_weight, second_weight]
    specs = [
        by_point,
        pl.BlockSpec(first_weight.shape, lambda i: (0, 0)),
        pl.BlockSpec(second_weight.shape, lambda i: (0, 0)),
    ]
    aliases = {}
    if acc is not None:
        operands.append(acc)
        specs.append(out_point)
        aliases = {3: 0}
    return pl.pallas_call(
        kernel,
        grid=(points,),
        in_specs=specs,
        out_specs=out_point,
        out_shape=jax.ShapeDtypeStruct((points, tokens, out_width), jnp.float32),
        input_output_aliases=aliases,
        name=name,
        cost_estimate=pl.CostEstimate(
            flops=flops,
            bytes_accessed=2 * (normed.size + first_weight.size + second_weight.size)
            + 8 * points * tokens * out_width,
            transcendentals=points * tokens * first_weight.shape[1],
        ),
    )(*operands)


def attention_shard(normed, qkv_shard, proj_shard, acc, head_count):
    rows, tokens = normed.shape[0] * normed.shape[1], normed.shape[1]
    flops = 2 * rows * (qkv_shard.size + proj_shard.size) + 8 * rows * tokens * head_count * 128
    kernel = functools.partial(attention_kernel, head_count, acc is None)
    return shard_call(kernel, normed, qkv_shard, proj_shard, acc, "attention_shard", flops)


def mlp_shard(normed, fc1_shard, fc2_shard, acc):
    rows = normed.shape[0] * normed.shape[1]
    flops = 2 * rows * (fc1_shard.size + fc2_shard.size)
    kernel = functools.partial(mlp_kernel, acc is None)
    return shard_call(kernel, normed, fc1_shard, fc2_shard, acc, "mlp_shard", flops)


def over_tm(weights, count):
    def swap(array, bit):
        return lax.ppermute(array, "tm", [(i, i ^ bit) for i in range(count)])

    held = [weights]
    bit = 2
    while bit < count:
        held = held + [tuple(swap(w, bit) for w in shard) for shard in held]
        bit *= 2
    out = []
    for shard in held:
        out.append(shard)
        if count > 1:
            out.append(tuple(swap(w, 1) for w in shard))
    return out


def forward(patch_rows, modulation, w_patch, w_final, attention_fn, mlp_fn):
    point_count, lat_count = patch_rows.shape
    patch_size = w_patch.shape[0]
    model_width = w_patch.shape[1]
    token_count = lat_count // patch_size
    tokens = jnp.dot(
        patch_rows.reshape(point_count * token_count, patch_size),
        w_patch,
        preferred_element_type=jnp.float32,
    )
    tokens = (
        tokens.reshape(point_count, token_count, model_width) + position_table(token_count)[None]
    )
    mod_float = modulation.astype(jnp.float32)[:, None, :]
    mod_parts = [
        mod_float[:, :, block_index * model_width : (block_index + 1) * model_width]
        for block_index in range(8)
    ]
    normed = (
        (layer_norm(tokens) * (1.0 + mod_parts[1]) + mod_parts[0])
        .astype(jnp.bfloat16)
    )
    mixed = tokens + mod_parts[2] * attention_fn(normed).reshape(
        point_count, token_count, model_width
    )
    normed_two = (
        (layer_norm(mixed) * (1.0 + mod_parts[4]) + mod_parts[3])
        .astype(jnp.bfloat16)
    )
    residual = mixed + mod_parts[5] * mlp_fn(normed_two).reshape(
        point_count, token_count, model_width
    )
    final_in = (
        (layer_norm(residual) * (1.0 + mod_parts[7]) + mod_parts[6])
        .astype(jnp.bfloat16)
        .reshape(-1, model_width)
    )
    return (
        jnp.dot(final_in, w_final, preferred_element_type=jnp.float32)
        .astype(jnp.bfloat16)
        .reshape(point_count, lat_count)
    )


def add_pair(earlier, later):
    return earlier + later


def local(
    latents,
    shifts,
    starts,
    labels,
    class_table,
    w_freq,
    w_time,
    w_ada,
    w_patch,
    w_qkv,
    w_proj,
    w_fc1,
    w_fc2,
    w_final,
):
    tm_count = lax.axis_size("tm")
    tm_index = lax.axis_index("tm")
    batch_index = lax.axis_index("batch")
    local_steps = latents.shape[0]
    window = local_steps * tm_count
    whole = lax.all_gather(latents, "tm", axis=0, tiled=True)
    local_positions = tm_index * local_steps + jnp.arange(local_steps, dtype=jnp.int32)[:, None]
    source_rows = jnp.minimum(local_positions + shifts[None, :], window - 1)
    points = jnp.take_along_axis(whole, source_rows[:, :, None], axis=0)
    anchor = jnp.take_along_axis(whole, shifts[None, :, None], axis=0)[0]
    by_sample = lax.all_to_all(
        points.astype(jnp.bfloat16), "batch", split_axis=1, concat_axis=2, tiled=True
    )
    sample_count = by_sample.shape[1]
    lat_count = by_sample.shape[2]
    own_shifts = lax.dynamic_slice_in_dim(shifts, batch_index * sample_count, sample_count)
    own_starts = lax.dynamic_slice_in_dim(starts, batch_index * sample_count, sample_count)
    own_labels = lax.dynamic_slice_in_dim(labels, batch_index * sample_count, sample_count)
    window_positions = jnp.arange(window, dtype=jnp.int32)[:, None]
    step_ids = (own_starts + own_shifts)[None, :] + window_positions
    class_ids = jnp.broadcast_to(own_labels[None, :], step_ids.shape)
    activation = cond_activation(
        step_ids.reshape(-1), class_ids.reshape(-1), class_table, w_freq, w_time
    )
    own_columns = jnp.dot(activation, w_ada, preferred_element_type=jnp.float32).astype(
        jnp.bfloat16
    )
    modulation = lax.all_to_all(own_columns, "tm", split_axis=0, concat_axis=1, tiled=True)
    point_rows = by_sample.reshape(local_steps * sample_count, lat_count)
    point_count = point_rows.shape[0]
    qkv_width = w_qkv.shape[1]
    entry = jnp.concatenate([w_qkv, w_proj.T], axis=1)
    entry = lax.all_gather(entry, "batch", axis=0, tiled=True)
    fc1_own = lax.all_gather(w_fc1, "batch", axis=0, tiled=True)
    fc2_own = lax.all_gather(w_fc2.T, "batch", axis=0, tiled=True).T
    attention_shards = over_tm((entry[:, :qkv_width], entry[:, qkv_width:].T), tm_count)
    mlp_shards = over_tm((fc1_own, fc2_own), tm_count)

    def attention_fn(normed):
        acc = None
        for qkv_shard, proj_shard in attention_shards:
            acc = attention_shard(normed, qkv_shard, proj_shard, acc, HEADS // tm_count)
        return acc

    def mlp_fn(normed_two):
        acc = None
        for fc1_shard, fc2_shard in mlp_shards:
            acc = mlp_shard(normed_two, fc1_shard, fc2_shard, acc)
        return acc

    velocity_mid = forward(point_rows, modulation, w_patch, w_final, attention_fn, mlp_fn)
    velocity_mid = velocity_mid.reshape(local_steps, sample_count, lat_count)
    velocity_out = lax.all_to_all(velocity_mid, "batch", split_axis=2, concat_axis=1, tiled=True)
    velocity_float = velocity_out.astype(jnp.float32)
    summed = jnp.cumsum(velocity_float, axis=0)
    running = jnp.concatenate([jnp.zeros_like(summed[:1]), summed[:-1]], axis=0)
    block_sum = jnp.sum(velocity_float, axis=0)
    earlier_sum = entering(block_sum, "tm", add_pair, jnp.zeros_like(block_sum))
    latents_out = anchor[None] + (earlier_sum[None] + running) * (1.0 / STEPS)
    return (latents_out, velocity_out)


def solution(mesh):
    placed = (
        P("tm", None, "batch"),
        P(),
        P(),
        P(),
        P(),
        P(),
        P(),
        P(None, "tm"),
        P(),
        P("batch", "tm"),
        P("tm", "batch"),
        P("batch", "tm"),
        P("tm", "batch"),
        P(),
    )
    return jax.shard_map(
        local,
        mesh=mesh,
        in_specs=placed,
        out_specs=(P("tm", None, "batch"), P("tm", None, "batch")),
        check_vma=False,
    )
```

```python
import functools
import math

import jax
import jax.numpy as jnp
from jax import lax
from jax.experimental import pallas as pl
from jax.sharding import PartitionSpec as P

D = 1152
HEADS = 16
FREQ = 256
GRID = 16
STEPS = 18


def entering(part, axis, combine, identity):
    place = lax.axis_index(axis)
    gathered = lax.all_gather(part, axis)
    state = jnp.zeros_like(part) + jnp.asarray(identity, part.dtype)

    def one(lap, state):
        return combine(state, lax.dynamic_index_in_dim(gathered, lap, 0, False))

    return lax.fori_loop(0, place, one, state)


def layer_norm(values):
    average = jnp.mean(values, axis=-1, keepdims=True)
    centred = values - average
    variance = jnp.mean(centred * centred, axis=-1, keepdims=True)
    return centred * lax.rsqrt(variance + 1e-06)


def position_table(token_count):
    token_ids = jnp.arange(token_count, dtype=jnp.int32)
    row_ids = (token_ids // GRID).astype(jnp.float32)
    col_ids = (token_ids % GRID).astype(jnp.float32)
    quarter = D // 4
    omegas = jnp.exp(-math.log(10000.0) * jnp.arange(quarter, dtype=jnp.float32) / quarter)
    col_angle = col_ids[:, None] * omegas[None, :]
    row_angle = row_ids[:, None] * omegas[None, :]
    return jnp.concatenate(
        [jnp.sin(col_angle), jnp.cos(col_angle), jnp.sin(row_angle), jnp.cos(row_angle)], axis=1
    )


def cond_activation(step_ids, class_ids, class_table, w_freq, w_time):
    half_freq = FREQ // 2
    freqs = jnp.exp(-math.log(10000.0) * jnp.arange(half_freq, dtype=jnp.float32) / half_freq)
    tvalue = 1000.0 * (1.0 - step_ids.astype(jnp.float32) / STEPS)
    angles = tvalue[:, None] * freqs[None, :]
    embedded = jnp.concatenate([jnp.cos(angles), jnp.sin(angles)], axis=1).astype(jnp.bfloat16)
    hidden_time = jax.nn.silu(jnp.dot(embedded, w_freq, preferred_element_type=jnp.float32)).astype(
        jnp.bfloat16
    )
    condition = jnp.dot(hidden_time, w_time, preferred_element_type=jnp.float32) + jnp.take(
        class_table, class_ids, axis=0
    ).astype(jnp.float32)
    return jax.nn.silu(condition).astype(jnp.bfloat16)


def times_transposed(left, right):
    return lax.dot_general(
        left, right, (((1,), (1,)), ((), ())), preferred_element_type=jnp.float32
    )


def attention_kernel(head_count, head_size, first, normed_ref, entry_ref, *rest):
    acc_ref, out_ref = (None, rest[0]) if first else rest
    qkv_width = 3 * head_count * head_size
    boundary = qkv_width // 128 * 128
    rows = jnp.dot(
        normed_ref[0], entry_ref[:, :qkv_width], preferred_element_type=jnp.float32
    )
    rows = rows.astype(jnp.bfloat16)
    scale = 1.0 / math.sqrt(head_size)
    pieces = []
    if qkv_width > boundary:
        pieces.append(jnp.zeros((rows.shape[0], qkv_width - boundary), jnp.bfloat16))
    for head in range(head_count):
        start = head * 3 * head_size
        query = rows[:, start : start + head_size]
        keys = rows[:, start + head_size : start + 2 * head_size]
        values = rows[:, start + 2 * head_size : start + 3 * head_size]
        scores = times_transposed(query, keys)
        peak = jnp.max(scores, axis=-1, keepdims=True)
        weights = jnp.exp((scores - peak) * scale)
        total = jnp.sum(weights, axis=-1, keepdims=True)
        mixed = jnp.dot(
            weights.astype(jnp.bfloat16), values, preferred_element_type=jnp.float32
        )
        pieces.append((mixed / total).astype(jnp.bfloat16))
    attended = jnp.concatenate(pieces, axis=1)
    product = times_transposed(attended, entry_ref[:, boundary:])
    out_ref[0] = product if first else acc_ref[0] + product


def mlp_kernel(first, normed_ref, fc1_ref, fc2_ref, *rest):
    acc_ref, out_ref = (None, rest[0]) if first else rest
    hidden = jnp.dot(normed_ref[0], fc1_ref[...], preferred_element_type=jnp.float32)
    hidden = jax.nn.gelu(hidden, approximate=True).astype(jnp.bfloat16)
    product = times_transposed(hidden, fc2_ref[...])
    out_ref[0] = product if first else acc_ref[0] + product


def shard_call(kernel, normed, weights, acc, name, flops, exps):
    points, tokens, width = normed.shape
    by_point = pl.BlockSpec((1, tokens, width), lambda i: (i, 0, 0))
    operands = [normed, *weights]
    specs = [by_point] + [pl.BlockSpec(w.shape, lambda i: (0, 0)) for w in weights]
    aliases = {}
    if acc is not None:
        aliases = {len(operands): 0}
        operands.append(acc)
        specs.append(by_point)
    return pl.pallas_call(
        kernel,
        grid=(points,),
        in_specs=specs,
        out_specs=by_point,
        out_shape=jax.ShapeDtypeStruct((points, tokens, width), jnp.float32),
        input_output_aliases=aliases,
        name=name,
        cost_estimate=pl.CostEstimate(
            flops=flops,
            bytes_accessed=2 * sum(w.size for w in weights) + 10 * normed.size,
            transcendentals=exps,
        ),
    )(*operands)


def attention_shard(normed, entry, acc, head_count):
    points, tokens, width = normed.shape
    rows, head_size = points * tokens, width // HEADS
    flops = 2 * rows * entry.size + 8 * rows * tokens * head_count * 128
    kernel = functools.partial(attention_kernel, head_count, head_size, acc is None)
    exps = rows * tokens * head_count
    return shard_call(kernel, normed, (entry,), acc, "attention_shard", flops, exps)


def mlp_shard(normed, fc1_shard, fc2_shard, acc):
    rows = normed.shape[0] * normed.shape[1]
    flops = 2 * rows * (fc1_shard.size + fc2_shard.size)
    kernel = functools.partial(mlp_kernel, acc is None)
    exps = rows * fc1_shard.shape[1]
    return shard_call(kernel, normed, (fc1_shard, fc2_shard), acc, "mlp_shard", flops, exps)


def over_tm(weights, count):
    def swap(array, bit):
        return lax.ppermute(array, "tm", [(i, i ^ bit) for i in range(count)])

    held = [weights]
    bit = 2
    while bit < count:
        held = held + [tuple(swap(w, bit) for w in shard) for shard in held]
        bit *= 2
    out = []
    for shard in held:
        out.append(shard)
        if count > 1:
            out.append(tuple(swap(w, 1) for w in shard))
    return out


def forward(patch_rows, modulation, w_patch, w_final, attention_fn, mlp_fn):
    point_count, lat_count = patch_rows.shape
    patch_size = w_patch.shape[0]
    model_width = w_patch.shape[1]
    token_count = lat_count // patch_size
    tokens = jnp.dot(
        patch_rows.reshape(point_count * token_count, patch_size),
        w_patch,
        preferred_element_type=jnp.float32,
    )
    tokens = (
        tokens.reshape(point_count, token_count, model_width) + position_table(token_count)[None]
    )
    mod_float = modulation.astype(jnp.float32)[:, None, :]
    mod_parts = [
        mod_float[:, :, block_index * model_width : (block_index + 1) * model_width]
        for block_index in range(8)
    ]
    normed = (
        (layer_norm(tokens) * (1.0 + mod_parts[1]) + mod_parts[0])
        .astype(jnp.bfloat16)
    )
    mixed = tokens + mod_parts[2] * attention_fn(normed).reshape(
        point_count, token_count, model_width
    )
    normed_two = (
        (layer_norm(mixed) * (1.0 + mod_parts[4]) + mod_parts[3])
        .astype(jnp.bfloat16)
    )
    residual = mixed + mod_parts[5] * mlp_fn(normed_two).reshape(
        point_count, token_count, model_width
    )
    final_in = (
        (layer_norm(residual) * (1.0 + mod_parts[7]) + mod_parts[6])
        .astype(jnp.bfloat16)
        .reshape(-1, model_width)
    )
    return (
        jnp.dot(final_in, w_final, preferred_element_type=jnp.float32)
        .astype(jnp.bfloat16)
        .reshape(point_count, lat_count)
    )


def add_pair(earlier, later):
    return earlier + later


def local(
    latents,
    shifts,
    starts,
    labels,
    class_table,
    w_freq,
    w_time,
    w_ada,
    w_patch,
    w_qkv,
    w_proj,
    w_fc1,
    w_fc2,
    w_final,
):
    tm_count = lax.axis_size("tm")
    tm_index = lax.axis_index("tm")
    batch_index = lax.axis_index("batch")
    local_steps = latents.shape[0]
    window = local_steps * tm_count
    whole = lax.all_gather(latents, "tm", axis=0, tiled=True)
    local_positions = tm_index * local_steps + jnp.arange(local_steps, dtype=jnp.int32)[:, None]
    source_rows = jnp.minimum(local_positions + shifts[None, :], window - 1)
    points = jnp.take_along_axis(whole, source_rows[:, :, None], axis=0)
    anchor = jnp.take_along_axis(whole, shifts[None, :, None], axis=0)[0]
    by_sample = lax.all_to_all(
        points.astype(jnp.bfloat16), "batch", split_axis=1, concat_axis=2, tiled=True
    )
    sample_count = by_sample.shape[1]
    lat_count = by_sample.shape[2]
    own_shifts = lax.dynamic_slice_in_dim(shifts, batch_index * sample_count, sample_count)
    own_starts = lax.dynamic_slice_in_dim(starts, batch_index * sample_count, sample_count)
    own_labels = lax.dynamic_slice_in_dim(labels, batch_index * sample_count, sample_count)
    window_positions = jnp.arange(window, dtype=jnp.int32)[:, None]
    step_ids = (own_starts + own_shifts)[None, :] + window_positions
    class_ids = jnp.broadcast_to(own_labels[None, :], step_ids.shape)
    activation = cond_activation(
        step_ids.reshape(-1), class_ids.reshape(-1), class_table, w_freq, w_time
    )
    own_columns = jnp.dot(activation, w_ada, preferred_element_type=jnp.float32).astype(
        jnp.bfloat16
    )
    modulation = lax.all_to_all(own_columns, "tm", split_axis=0, concat_axis=1, tiled=True)
    point_rows = by_sample.reshape(local_steps * sample_count, lat_count)
    point_count = point_rows.shape[0]
    entry = jnp.concatenate([w_qkv, w_proj.T], axis=1)
    entry = lax.all_gather(entry, "batch", axis=0, tiled=True)
    fc1_own = lax.all_gather(w_fc1, "batch", axis=0, tiled=True)
    fc2_own = lax.all_gather(w_fc2.T, "batch", axis=0, tiled=True)
    attention_shards = over_tm((entry,), tm_count)
    mlp_shards = over_tm((fc1_own, fc2_own), tm_count)

    def attention_fn(normed):
        acc = None
        for (entry_shard,) in attention_shards:
            acc = attention_shard(normed, entry_shard, acc, HEADS // tm_count)
        return acc

    def mlp_fn(normed_two):
        acc = None
        for fc1_shard, fc2_shard in mlp_shards:
            acc = mlp_shard(normed_two, fc1_shard, fc2_shard, acc)
        return acc

    velocity_mid = forward(point_rows, modulation, w_patch, w_final, attention_fn, mlp_fn)
    velocity_mid = velocity_mid.reshape(local_steps, sample_count, lat_count)
    velocity_out = lax.all_to_all(velocity_mid, "batch", split_axis=2, concat_axis=1, tiled=True)
    velocity_float = velocity_out.astype(jnp.float32)
    summed = jnp.cumsum(velocity_float, axis=0)
    running = jnp.concatenate([jnp.zeros_like(summed[:1]), summed[:-1]], axis=0)
    block_sum = jnp.sum(velocity_float, axis=0)
    earlier_sum = entering(block_sum, "tm", add_pair, jnp.zeros_like(block_sum))
    latents_out = anchor[None] + (earlier_sum[None] + running) * (1.0 / STEPS)
    return (latents_out, velocity_out)


def solution(mesh):
    placed = (
        P("tm", None, "batch"),
        P(),
        P(),
        P(),
        P(),
        P(),
        P(),
        P(None, "tm"),
        P(),
        P("batch", "tm"),
        P("tm", "batch"),
        P("batch", "tm"),
        P("tm", "batch"),
        P(),
    )
    return jax.shard_map(
        local,
        mesh=mesh,
        in_specs=placed,
        out_specs=(P("tm", None, "batch"), P("tm", None, "batch")),
        check_vma=False,
    )
```
